8 devices in a mesh: rep: 2 (over y, z), dp: 4 (over x, core).
Axes of the slice: x: 2, y: 2, z: 1, core: 2. Of those that a mesh axis runs over, the one named last changes fastest.
Arguments:
- x: bfloat16 [8, 2048, 1280], P(('rep', 'dp')), parts along dimension 0
- dy: bfloat16 [8, 2048, 1280], P(('rep', 'dp')), parts along dimension 0
- w_gate: bfloat16 [2, 1280, 4480], P(None, 'dp')
- w_up: bfloat16 [2, 1280, 4480], P(None, 'dp')
- w_down: bfloat16 [2, 4480, 1280], P(None, 'dp')
- m_w_gate: float32 [2, 1280, 4480], P(None, 'dp')
- m_w_up: float32 [2, 1280, 4480], P(None, 'dp')
- m_w_down: float32 [2, 4480, 1280], P(None, 'dp')
- v_w_gate: float32 [2, 1280, 4480], P(None, 'dp')
- v_w_up: float32 [2, 1280, 4480], P(None, 'dp')
- v_w_down: float32 [2, 4480, 1280], P(None, 'dp')
Outputs:
- output 1: bfloat16 [4, 1280, 4480], P('rep', 'dp'), parts along dimension 0
- output 2: bfloat16 [4, 1280, 4480], P('rep', 'dp'), parts along dimension 0
- output 3: bfloat16 [4, 4480, 1280], P('rep', 'dp'), parts along dimension 0
- output 4: float32 [4, 1280, 4480], P('rep', 'dp'), parts along dimension 0
- output 5: float32 [4, 1280, 4480], P('rep', 'dp'), parts along dimension 0
- output 6: float32 [4, 4480, 1280], P('rep', 'dp'), parts along dimension 0
- output 7: float32 [4, 1280, 4480], P('rep', 'dp'), parts along dimension 0
- output 8: float32 [4, 1280, 4480], P('rep', 'dp'), parts along dimension 0
- output 9: float32 [4, 4480, 1280], P('rep', 'dp'), parts along dimension 0
There are 2 independent parts. The reference program is written for one: setup_inputs(seed, part) draws one part's arguments, and reference() takes and returns one part's arrays. A program takes and returns all parts, laid end to end along the dimension named above; an argument that names none is the same for every part.
All inputs are finite; a program needn't handle non-finite values.
Results may differ from the reference program's by a relative error of at most 0.022.
Values are sent between devices in bfloat16 or wider.
A program may use at most 2 GiB of HBM per device.

```python
import jax
import jax.numpy as jnp
from jax import lax

SEQUENCES = 4
TOKENS = 2048
D = 1280
FF = 4480
LAYERS = 2
NAMES = ("w_gate", "w_up", "w_down")
SHAPES = {"w_gate": (LAYERS, D, FF), "w_up": (LAYERS, D, FF), "w_down": (LAYERS, FF, D)}


def bump(key, n, height):
    away = (jnp.arange(n, dtype=jnp.int32) - jax.random.randint(key, (), 0, n, jnp.int32)) % n
    return jnp.where(away < n // 8, height, 1.0)


def together(key, own, strength):
    shared = jax.random.normal(key, own.shape[1:], jnp.float32)
    return (own + strength * shared) * lax.rsqrt(1 + strength * strength)


def setup_inputs(seed: int = 0, part: int = 0) -> dict:
    kx, kdy, ka, kb, kz, kf, kh, kl, *keys = jax.random.split(jax.random.key(seed), 8 + 3 * len(NAMES))
    kx, kdy, ka, kb = (jax.random.fold_in(k, part) for k in (kx, kdy, ka, kb))
    kw, km, kv = (keys[i::3] for i in range(3))
    shape = (SEQUENCES, TOKENS, D)
    much_x, much_dy = jax.random.uniform(kz, (2,), jnp.float32, 0.0, 1.0)
    loud = 2.0 ** jax.random.uniform(jax.random.fold_in(kz, 1), (), jnp.float32, -1.0, 2.0)
    layers = 2.0 ** jax.random.uniform(kl, (LAYERS, 1, 1), jnp.float32, -1.0, 1.0)
    x = together(ka, jax.random.normal(kx, shape, jnp.float32), much_x) * bump(kf, D, 4.0)
    dy = together(kb, jax.random.normal(kdy, shape, jnp.float32), much_dy)
    drawn = {"x": x.astype(jnp.bfloat16), "dy": (loud * dy * (SEQUENCES * TOKENS) ** -0.5).astype(jnp.bfloat16)}
    for key, name in zip(kw, NAMES, strict=True):
        w = jax.random.normal(key, SHAPES[name], jnp.float32) * SHAPES[name][1] ** -0.5
        drawn[name] = (w * {"w_gate": 1.0, "w_up": bump(kh, FF, 4.0), "w_down": layers}[name]).astype(jnp.bfloat16)
    for key, name in zip(km, NAMES, strict=True):
        drawn[f"m_{name}"] = 0.1 * jax.random.normal(key, SHAPES[name], jnp.float32)
    for key, name in zip(kv, NAMES, strict=True):
        drawn[f"v_{name}"] = jax.random.uniform(key, SHAPES[name], jnp.float32, 0.005, 0.015)
    return drawn


def matmul(a, w):
    return jnp.dot(a, w, preferred_element_type=jnp.float32).astype(jnp.bfloat16)


def normed(h):
    wide = h.astype(jnp.float32)
    scale = lax.rsqrt(jnp.mean(wide**2, -1, keepdims=True) + 1e-6)
    return (wide * scale).astype(jnp.bfloat16)


def layer(h, w):
    a = normed(h)
    gate = jnp.dot(a, w["w_gate"], preferred_element_type=jnp.float32)
    up = jnp.dot(a, w["w_up"], preferred_element_type=jnp.float32)
    return h + matmul((jax.nn.silu(gate) * up).astype(jnp.bfloat16), w["w_down"])


def adamw(w, m, v, g):
    m = 0.9 * m + 0.1 * g
    v = 0.95 * v + 0.05 * g * g
    step = m * lax.rsqrt(v + 1e-8) + 0.1 * w
    return (w - 0.02 * step).astype(jnp.bfloat16), m, v


def stack(weights, h):
    return lax.scan(lambda h, w: (layer(h, w), None), h, weights)[0]


def reference(x, dy, w_gate, w_up, w_down, m_w_gate, m_w_up, m_w_down, v_w_gate, v_w_up, v_w_down):
    weights = dict(zip(NAMES, (w_gate, w_up, w_down), strict=True))

    def take(so_far, sequence):
        h, by_y = sequence
        _, back = jax.vjp(lambda w: stack(w, h), weights)
        return jax.tree.map(lambda total, term: total + term.astype(jnp.float32), so_far, back(by_y)[0]), None

    none_yet = {name: jnp.zeros(w.shape, jnp.float32) for name, w in weights.items()}
    by_weights, _ = lax.scan(take, none_yet, (x, dy))
    gradients = [by_weights[name].astype(jnp.bfloat16).astype(jnp.float32) for name in NAMES]
    new = [
        adamw(w.astype(jnp.float32), m, v, g)
        for w, m, v, g in zip((w_gate, w_up, w_down), (m_w_gate, m_w_up, m_w_down), (v_w_gate, v_w_up, v_w_down), gradients, strict=True)
    ]
    return tuple(one[which] for which in range(3) for one in new)
```

```python
import jax
import jax.numpy as jnp
from jax import lax
from jax.experimental import pallas as pl
from jax.experimental.pallas import tpu as pltpu
from jax.sharding import PartitionSpec as P


MESH = pl.DeviceIdType.MESH
HBM = pl.BlockSpec(memory_space=pltpu.HBM)
TILE = 512
CHUNK = 1024
BLOCK = 256
LAYERS = 2
COUNT = 3 * LAYERS


def cuts(rows):
    units = rows // 16
    small = max(units // 10, 1)
    middle = units - 2 * small
    sizes = [small] + [middle // 4 + (k < middle % 4) for k in range(4)] + [small]
    starts = [sum(sizes[:k]) for k in range(len(sizes))]
    return [(16 * a, 16 * b) for a, b in zip(starts, sizes)]


PIECES = 6
AHEAD = 8
LEAD = 2


class Gather:
    def __init__(self, blocks, wholes, sems):
        self.blocks, self.wholes = blocks, wholes
        self.own_s, self.own_r, self.x_s, self.x_r, self.y_s, self.y_r, self.c_s, self.c_r, self.e_s, self.e_r = sems
        y, d = lax.axis_index("rep"), lax.axis_index("dp")
        self.y, self.x, self.c = y, d // 2, d % 2
        self.over_x, self.over_y, self.over_c = (y, (1 - self.x) * 2 + self.c), (1 - y, d), (y, self.x * 2 + 1 - self.c)

    def barrier(self):
        sem = pltpu.get_barrier_semaphore()
        for device in (self.over_x, self.over_y, self.over_c):
            pl.semaphore_signal(sem, inc=1, device_id=device, device_id_type=MESH)
        pl.semaphore_wait(sem, 3)

    def mine(self, j):
        rows = self.blocks[j].shape[0]
        return self.wholes[j].at[pl.ds((self.x * 2 + self.c) * rows, rows)]

    def own(self, j):
        return pltpu.make_async_remote_copy(
            self.blocks[j], self.mine(j), self.own_s.at[j], self.own_r.at[j], device_id=self.over_c, device_id_type=MESH
        )

    def piece(self, j, k, chip, half):
        rows = self.blocks[j].shape[0]
        start, size = cuts(rows // 2)[k]
        return self.wholes[j].at[pl.ds((chip * 2 + self.c) * rows + half * (rows // 2) + start, size)]

    def first(self, j, k):
        rows = self.blocks[j].shape[0]
        start, size = cuts(rows // 2)[k]
        source = self.blocks[j].at[pl.ds(self.y * (rows // 2) + start, size)]
        n = j * PIECES + k
        return pltpu.make_async_remote_copy(
            source, self.piece(j, k, self.x, self.y), self.x_s.at[n], self.x_r.at[n], device_id=self.over_x, device_id_type=MESH
        )

    def send(self, j, k, half, sems, device):
        at, n = self.piece(j, k, 1 - self.x, half), j * PIECES + k
        return pltpu.make_async_remote_copy(at, at, sems[0].at[n], sems[1].at[n], device_id=device, device_id_type=MESH)

    def second(self, j, k):
        return self.send(j, k, self.y, (self.y_s, self.y_r), self.over_y)

    def hand(self, j, k):
        return self.send(j, k, self.y, (self.c_s, self.c_r), self.over_c)

    def hand_late(self, j, k):
        return self.send(j, k, 1 - self.y, (self.e_s, self.e_r), self.over_c)

    def start(self):
        self.barrier()
        for n in range(AHEAD):
            self.first(*divmod(n, PIECES)).start()
        for j in range(len(self.blocks)):
            self.own(j).start()

    def pass_on(self, n):
        at = divmod(n, PIECES)
        self.first(*at).wait()
        if n + AHEAD < len(self.blocks) * PIECES:
            self.first(*divmod(n + AHEAD, PIECES)).start()
        self.second(*at).start()
        self.hand(*at).start()
        if n >= 1:
            self.pass_late(n - 1)

    def pass_late(self, n):
        j, k = divmod(n, PIECES)
        self.send(j, k, 1 - self.y, (self.y_s, self.y_r), self.over_y).wait_recv()
        self.hand_late(j, k).start()

    def ready(self, j):
        self.own(j).wait_recv()
        for k in range(PIECES):
            self.hand(j, k).wait_recv()
            self.hand_late(j, k).wait_recv()

    def finish(self):
        for j in range(len(self.blocks)):
            self.own(j).wait_send()
            for k in range(PIECES):
                self.second(j, k).wait_send()
                self.hand(j, k).wait_send()
                self.hand_late(j, k).wait_send()


def scaled(wide):
    return (wide * lax.rsqrt(jnp.mean(wide * wide, -1, keepdims=True) + 1e-6)).astype(jnp.bfloat16)


def dot(a, b):
    return jnp.dot(a, b, preferred_element_type=jnp.float32)


def chunks(rows, body):
    @pl.loop(0, rows // CHUNK)
    def _(n):
        body(pl.ds(pl.multiple_of(n * CHUNK, CHUNK), CHUNK))


def over_columns(body, ins, outs, tick):
    columns = ins[0].shape[1]
    main = columns // TILE
    steps = pl.cdiv(columns, TILE)
    for start, count, width in ((0, main, TILE), (main * TILE, steps - main, columns - main * TILE)):
        if count == 0:
            continue

        def tile(*refs, start=start, width=width):
            n = pl.program_id(0)
            tick(start // TILE + n, steps)
            body(pl.ds(pl.multiple_of(start + n * width, 128), width), *refs)

        specs = [pl.BlockSpec((r.shape[0], width), lambda n: (0, n)) for r in ins + outs]
        parts = [r.at[:, pl.ds(start, count * width)] for r in ins + outs]
        pltpu.emit_pipeline(tile, grid=(count,), in_specs=specs[: len(ins)], out_specs=specs[len(ins) :])(*parts)


def forward_kernel(x_ref, wg, wu, wd, g0, u0, d0, g1, u1, d1, a0_ref, a1_ref, h1_ref, gate0, up0, hid0, gate1, up1, hid1, act, sem, out_sem, *sems):
    blocks = [w.at[n] for n in range(LAYERS) for w in (wg, wu, wd)]
    wholes = [g0, u0, d0, g1, u1, d1]
    g = Gather(blocks, wholes, sems)
    g.start()

    def ticks(j):
        def tick(n, steps):
            for k in range(PIECES):
                piece = j * PIECES + LEAD + k
                if piece < COUNT * PIECES:

                    @pl.when(n == (k + 1) * (steps - 1) // PIECES)
                    def _(piece=piece):
                        g.pass_on(piece)

        return tick

    def place_own(wide_block, tall_block):
        for j in range(COUNT):
            g.pass_on(j)
            held = tall_block if j % 3 == 2 else wide_block
            for source, target in ((blocks[j], held), (held, g.mine(j))):
                move = pltpu.make_async_copy(source, target, sem.at[1])
                move.start()
                move.wait()

    copy = pltpu.make_async_copy(x_ref, act, sem.at[0])
    copy.start()
    copy.wait()
    chunks(act.shape[0], lambda rows: act.__setitem__((rows, slice(None)), scaled(act[rows, :].astype(jnp.float32))))
    copy = pltpu.make_async_copy(act, a0_ref, sem.at[0])
    copy.start()
    pl.run_scoped(place_own, pltpu.VMEM(blocks[0].shape, blocks[0].dtype), pltpu.VMEM(blocks[2].shape, blocks[2].dtype))
    for n in range(COUNT, PIECES + LEAD):
        g.pass_on(n)
    g.ready(0)
    copy.wait()

    def gate_and_up(j, w_gate, w_up, gate_ref, up_ref, hid_ref):
        def within(gate):
            def gate_tile(columns, w):
                def some(rows):
                    gate[rows, columns] = dot(act[rows, :], w[...])

                chunks(act.shape[0], some)
                pltpu.make_async_copy(gate.at[:, columns], gate_ref.at[:, columns], out_sem.at[0]).start()

            def up_tile(columns, w, up_out, hid):
                def some(rows):
                    up = dot(act[rows, :], w[...])
                    up_out[rows, :] = up
                    hid[rows, :] = (jax.nn.silu(gate[rows, columns]) * up).astype(jnp.bfloat16)

                chunks(act.shape[0], some)

            over_columns(gate_tile, [w_gate], [], ticks(j))
            g.ready(j)
            over_columns(up_tile, [w_up], [up_ref, hid_ref], ticks(j + 1))
            pltpu.make_async_copy(gate, gate_ref, out_sem.at[0]).wait()

        pl.run_scoped(within, pltpu.VMEM(gate_ref.shape, gate_ref.dtype))

    gate_and_up(1, g0, u0, gate0, up0, hid0)
    g.ready(2)

    def down(w_down):
        load = pltpu.make_async_copy(d0, w_down, sem.at[0])
        load.start()
        load.wait()
        steps = act.shape[0] // BLOCK

        def some(hid, x, h1, a1):
            ticks(3)(pl.program_id(0), steps)
            wide = x[...].astype(jnp.float32) + dot(hid[...], w_down[...]).astype(jnp.bfloat16).astype(jnp.float32)
            h = wide.astype(jnp.bfloat16)
            h1[...] = h
            a1[...] = scaled(h.astype(jnp.float32))

        rows = lambda r: pl.BlockSpec((BLOCK, r.shape[1]), lambda n: (n, 0))
        refs = (hid0, x_ref, h1_ref, a1_ref)
        pltpu.emit_pipeline(some, grid=(steps,), in_specs=[rows(r) for r in refs[:2]], out_specs=[rows(r) for r in refs[2:]])(*refs)

    pl.run_scoped(down, pltpu.VMEM(d0.shape, d0.dtype))
    copy = pltpu.make_async_copy(a1_ref, act, sem.at[0])
    copy.start()
    g.ready(3)
    copy.wait()
    gate_and_up(4, g1, u1, gate1, up1, hid1)
    g.pass_late(COUNT * PIECES - 1)
    g.ready(5)
    g.finish()


def forward(x, w_gate, w_up, w_down):
    (tokens, d), ff = x.shape, w_gate.shape[2]
    bf16, f32 = jnp.bfloat16, jnp.float32
    shape = jax.ShapeDtypeStruct
    wholes = [shape((d, ff), bf16), shape((d, ff), bf16), shape((ff, d), bf16)] * LAYERS
    states = [shape((tokens, d), bf16)] * 3
    hidden = [shape((tokens, ff), f32), shape((tokens, ff), f32), shape((tokens, ff), bf16)] * LAYERS
    pieces = COUNT * PIECES
    out = pl.pallas_call(
        forward_kernel,
        name="forward",
        out_shape=wholes + states + hidden,
        in_specs=[HBM] * 4,
        out_specs=[HBM] * (len(wholes) + len(states) + len(hidden)),
        scratch_shapes=[pltpu.VMEM((tokens, d), bf16), pltpu.SemaphoreType.DMA((2,)), pltpu.SemaphoreType.DMA((1,))]
        + [pltpu.SemaphoreType.DMA((n,)) for n in (COUNT, COUNT) + (pieces,) * 8],
        compiler_params=pltpu.CompilerParams(collective_id=0, has_side_effects=True, vmem_limit_bytes=63 * 2**20),
    )(x, w_gate, w_up, w_down)
    return out[:COUNT], out[COUNT : COUNT + 3], out[COUNT + 3 :]


def normed(h):
    return scaled(h.astype(jnp.float32))


def adamw(w, m, v, g):
    m = 0.9 * m + 0.1 * g
    v = 0.95 * v + 0.05 * g * g
    step = m * lax.rsqrt(v + 1e-8) + 0.1 * w
    return (w - 0.02 * step).astype(jnp.bfloat16), m, v


CORES = [[0, 1], [2, 3]]
OVER_X = [(0, 2), (1, 3), (2, 0), (3, 1)]


def summed(g):
    g = g.reshape(2, 2, g.shape[0] // 4, g.shape[1])
    return lax.psum_scatter(g, "dp", scatter_dimension=1, axis_index_groups=CORES)


def backward_hidden(by_h, w_down, gate, up):
    by_hid = lax.dot_general(by_h, w_down, (((1,), (1,)), ((), ())), preferred_element_type=jnp.float32).astype(jnp.bfloat16).astype(jnp.float32)
    s = jax.nn.sigmoid(gate)
    by_up = by_hid * (gate * s)
    by_gate = by_hid * up * (s * (1 + gate * (1 - s)))
    return by_gate.astype(jnp.bfloat16), by_up.astype(jnp.bfloat16)


def to_weight(a, b):
    return lax.dot_general(a, b, (((0,), (0,)), ((), ())), preferred_element_type=jnp.float32).astype(jnp.bfloat16)


def to_input(a, w):
    return lax.dot_general(a, w, (((1,), (1,)), ((), ())), preferred_element_type=jnp.float32)


def solution(mesh):
    def step(x, dy, *arrays):
        weights, m, v = (arrays[i : i + 3] for i in (0, 3, 6))
        chip = lax.axis_index("dp") // 2
        x, dy = x[0], dy[0]
        wholes, (a0, a1, h1), hidden = forward(x, *weights)
        (_, _, down0, gate1, up1, down1) = wholes
        summing, got = {}, {}

        def send(name, g):
            summing[name] = summed(g)

        def travel(name, *later):
            both, *later = lax.optimization_barrier((summing[name], *later))
            theirs, ours = (lax.dynamic_index_in_dim(both, at, 0, False) for at in (1 - chip, chip))
            got[name] = (ours, lax.ppermute(theirs, "dp", OVER_X))
            return later

        g, u, hid = hidden[3:]
        send("d1", to_weight(hid, dy))
        by_gate, by_up = backward_hidden(dy, down1, g, u)
        by_gate, by_up = travel("d1", by_gate, by_up)
        send("g1", to_weight(a1, by_gate))
        send("u1", to_weight(a1, by_up))
        by_gate, by_up = travel("g1", by_gate, by_up)
        by_a = (to_input(by_gate, gate1) + to_input(by_up, up1)).astype(jnp.bfloat16)
        by_h = dy + jax.vjp(normed, h1)[1](by_a)[0]
        (by_h,) = travel("u1", by_h)
        g, u, hid = hidden[:3]
        send("d0", to_weight(hid, by_h))
        by_gate, by_up = backward_hidden(by_h, down0, g, u)
        by_gate, by_up = travel("d0", by_gate, by_up)
        send("g0", to_weight(a0, by_gate))
        by_u0 = to_weight(a0, by_up)
        send("u0", by_u0)
        travel("g0", by_u0)
        travel("u0")

        new = []
        for name, w, m, v in zip("gud", weights, m, v):
            total = [(ours.astype(jnp.float32) + other.astype(jnp.float32)).astype(jnp.bfloat16) for ours, other in (got[name + "0"], got[name + "1"])]
            new.append(adamw(w.astype(jnp.float32), m, v, jnp.stack(total).astype(jnp.float32)))
        return tuple(one[which] for which in range(3) for one in new)

    states, cut = P(("rep", "dp"), None, None), P(None, "dp", None)
    return jax.shard_map(
        step,
        mesh=mesh,
        in_specs=(states, states) + (cut,) * 9,
        out_specs=(P("rep", "dp", None),) * 9,
        check_vma=False,
    )
```
